256 devices in a mesh: col: 16 (over x_lo, z), tile: 16 (over y, x_hi, core).
Axes of the slice: x: 4 (x_hi: 2, x_lo: 2; x = x_hi * 2 + x_lo), y: 4, z: 8, core: 2. Of those that a mesh axis runs over, the one named last changes fastest.
Arguments:
- initial_image: float32 [65536, 2048], P('tile', 'col'), may hold values from -6 to 6
- panels: float32 [16, 256, 65536], P('col', None, 'tile'), may hold values from -0.0234375 to 0.0234375
- sinogram: float32 [16, 256, 2048], P(None, 'tile', 'col'), may hold values from -6 to 6
- subset_order: int32 [3], replicated, may hold values from 0 to 15
- step_sizes: float32 [3], replicated, may hold values from 0.5 to 1
Outputs:
- final_image: float32 [65536, 2048], P('tile', 'col')
- final_duals: float32 [16, 256, 2048], P(None, 'tile', 'col')
The draws below stay inside these ranges and needn't reach their ends.
Inputs may be any that keep to these rules, and one draw needn't show every extreme that they name: `subset_order`: repeats may occur.
All inputs are finite; a program needn't handle non-finite values.
Results may differ from the reference program's by a relative error of at most 0.00013.
Values sent between devices are 32-bit elements; how exact they have to be, the bound alone decides.
A program may use at most 128 MiB of HBM per device.

```python
import jax
import jax.numpy as jnp
from jax import lax

WIDTH = 512
RSUB = 256
ITERS = 3
ROWS = 128
NPIX = 65536
CHANNELS = 2048
SUBSETS = 16


def block_levels(rng, shape, split, least, largest):
    gain = 1.0
    for axis_at, blocks in split:
        heights = jax.random.uniform(jax.random.fold_in(jax.random.fold_in(rng, 6), axis_at), (blocks,), jnp.float32, least / len(split), largest / len(split))
        gain = gain * jnp.repeat(jnp.exp(heights), shape[axis_at] // blocks).reshape((-1,) + (1,) * (len(shape) - 1 - axis_at))
    return gain


def scatter_about(key, dims, deviation, bound, pieces=(), kind=jnp.bfloat16):
    result = deviation * jax.random.normal(key, dims, jnp.float32)
    if pieces:
        result = result * block_levels(key, dims, pieces, -0.22, 0.18)
    return jnp.clip(result, -bound, bound).astype(kind)


def setup_inputs(seed: int = 0) -> dict:
    seeds = jax.random.split(jax.random.key(seed), 6)
    return {
        "initial_image": scatter_about(seeds[0], (NPIX, CHANNELS), 1.0, 6.0, ((0, 16), (1, 16)), jnp.float32),
        "panels": scatter_about(seeds[1], (SUBSETS, RSUB, NPIX), NPIX ** -0.5, 0.0234375, ((0, 16), (2, 16)), jnp.float32),
        "sinogram": scatter_about(seeds[2], (SUBSETS, RSUB, CHANNELS), 1.0, 6.0, ((1, 16), (2, 16)), jnp.float32),
        "subset_order": jax.random.randint(seeds[3], (ITERS,), 0, SUBSETS).astype(jnp.int32),
        "step_sizes": jnp.clip(jax.random.uniform(seeds[4], (3,), jnp.float32, 0.5, 1.0), 0.5, 1.0),
    }


penalty = 0.2
smoothing = 1.0

def divergence(image_field):
    channels = image_field.shape[2]
    row_zero = jnp.zeros((1, WIDTH, channels), image_field.dtype)
    column_zero = jnp.zeros((image_field.shape[0], 1, channels), image_field.dtype)
    downward = jnp.concatenate([image_field[1:] - image_field[:-1], row_zero], axis=0)
    across = jnp.concatenate([image_field[:, 1:] - image_field[:, :-1], column_zero], axis=1)
    magnitude = jnp.sqrt(across * across + downward * downward + smoothing * smoothing)
    flux_across = across / magnitude
    flux_down = downward / magnitude
    shifted_across = jnp.concatenate([column_zero, flux_across[:, :-1]], axis=1)
    shifted_down = jnp.concatenate([row_zero, flux_down[:-1]], axis=0)
    return flux_across - shifted_across + flux_down - shifted_down

def reference(initial_image, panels, sinogram, subset_order, step_sizes):
    dual_step = step_sizes[0]
    primal_step = step_sizes[1]
    extrapolate = step_sizes[2]

    def primal(estimate, extrapolated):
        field_div = divergence(estimate.reshape(ROWS, WIDTH, CHANNELS)).reshape(estimate.shape)
        return estimate - primal_step * extrapolated + primal_step * penalty * field_div
    estimate = initial_image
    dual_state = jnp.zeros(sinogram.shape, jnp.float32)
    accumulated = jnp.zeros(initial_image.shape, jnp.float32)
    extrapolated = jnp.zeros(initial_image.shape, jnp.float32)
    for iteration in range(ITERS):
        estimate = primal(estimate, extrapolated)
        subset = subset_order[iteration].astype(jnp.int32)
        operator_panel = lax.dynamic_index_in_dim(panels, subset, 0, keepdims=False)
        forward = jnp.dot(operator_panel, estimate, precision=lax.Precision.HIGHEST, preferred_element_type=jnp.float32)
        current = lax.dynamic_index_in_dim(dual_state, subset, 0, keepdims=False)
        measured = lax.dynamic_index_in_dim(sinogram, subset, 0, keepdims=False)
        updated = (current + dual_step * forward - dual_step * measured) / (1.0 + dual_step)
        change = updated - current
        dual_state = lax.dynamic_update_index_in_dim(dual_state, updated, subset, 0)
        adjoint = jnp.dot(operator_panel.T, change, precision=lax.Precision.HIGHEST, preferred_element_type=jnp.float32)
        accumulated = accumulated + adjoint
        extrapolated = accumulated + extrapolate * SUBSETS * adjoint
    final_image = primal(estimate, extrapolated)
    return (final_image, dual_state)
```

```python
import jax
import jax.numpy as jnp
from jax import lax
from jax.experimental import pallas as pl
from jax.experimental.pallas import tpu as pltpu
from jax.sharding import PartitionSpec as P

MESH = pl.DeviceIdType.MESH
WIDTH = 512
ITERS = 3
PENALTY = 0.2
RING = 8
LAG = 3
COUNTS = (11, 11, 10)
CHUNK = 4
CHUNKS = 88
STEPS = CHUNKS + 8 * LAG
SLOTS = 8
F32 = jnp.float32
BF16 = jnp.bfloat16
PLUS, MINUS, ACROSS, OWN = 0, 1, 2, 3


def halves(x):
    high = x.astype(BF16)
    return high, (x - high.astype(F32)).astype(BF16)


def matmul(a, b, dims):
    return lax.dot_general(a, b, (dims, ((), ())), preferred_element_type=F32)


def kernel(base, steps, image, panel, measured, turns, again, out, duals,
           recv, staging, u, w, acc, high, low, above, below, flux,
           fwd, shares, change_own, changes,
           recv_sem, send_sem, own_sem, halo_send, halo_recv, sum_send, sum_recv, all_send, all_recv):
    col, tile = lax.axis_index("col"), lax.axis_index("tile")
    tiles = lax.axis_size("tile")
    rail, z = col // RING, lax.rem(col, RING)
    up = rail * RING + lax.rem(z + 1, RING)
    down = rail * RING + lax.rem(z + RING - 1, RING)
    partner = (1 - rail) * RING + z
    next_tile, prev_tile = lax.rem(tile + 1, tiles), lax.rem(tile + tiles - 1, tiles)
    links = ((PLUS, up), (MINUS, down), (ACROSS, partner))

    blocks = panel.shape[3] // 128
    def own_copy(tree, block):
        count = COUNTS[tree]
        return pltpu.make_async_copy(
            panel.at[0, pl.ds(sum(COUNTS[:tree]), count), :,
                     pl.ds(pl.multiple_of(block * 128, 128), 128)],
            recv.at[OWN, tree, pl.ds(block * count, count)],
            own_sem.at[tree, block],
        )

    for tree in range(3):
        @pl.loop(0, blocks)
        def _(block, tree=tree):
            own_copy(tree, block).start()

    barrier = pltpu.get_barrier_semaphore()
    for _, where in links:
        pl.semaphore_signal(barrier, inc=1, device_id={"col": where}, device_id_type=MESH)
    for d in range(1, tiles):
        pl.semaphore_signal(
            barrier, inc=1, device_id={"tile": lax.rem(tile + d, tiles)}, device_id_type=MESH)
    pl.semaphore_wait(barrier, tiles + 2)

    def halo_copies(source, m):
        last = source.shape[0] - WIDTH
        return (
            pltpu.make_async_remote_copy(
                source.at[pl.ds(0, WIDTH)], below.at[m], halo_send.at[m, 0], halo_recv.at[m, 0],
                device_id={"tile": prev_tile}, device_id_type=MESH),
            pltpu.make_async_remote_copy(
                source.at[pl.ds(last, WIDTH)], above.at[m], halo_send.at[m, 1], halo_recv.at[m, 1],
                device_id={"tile": next_tile}, device_id_type=MESH),
        )

    for copy in halo_copies(image, 0):
        copy.start()

    for tree in range(3):
        @pl.loop(0, blocks)
        def _(block, tree=tree):
            own_copy(tree, block).wait()

    def hop(link, where, step, slot):
        return pltpu.make_async_remote_copy(
            staging.at[slot, link],
            recv.at[link, :, pl.ds(step * CHUNK, CHUNK)],
            send_sem.at[slot, link], recv_sem.at[slot, link],
            device_id={"col": where}, device_id_type=MESH)

    def arrival(link, step, slot):
        ref = recv.at[link, :, pl.ds(step * CHUNK, CHUNK)]
        return pltpu.make_async_copy(ref, ref, recv_sem.at[slot, link])

    def chunk(link, k, step):
        return recv[link, k, pl.ds(step * CHUNK, CHUNK)]

    for step in range(LAG):
        for tree, (link, where) in enumerate(links):
            for k in range(ITERS):
                staging[step, link, k] = chunk(OWN, tree, step)
        for link, where in links:
            hop(link, where, step, step).start()

    @pl.loop(LAG, STEPS)
    def _(step):
        slot = lax.rem(step, SLOTS)
        came = step - LAG
        for link, _ in links:
            arrival(link, came, lax.rem(came, SLOTS)).wait()

        @pl.when(step >= SLOTS)
        def _():
            for link, where in links:
                hop(link, where, step - SLOTS, slot).wait_send()

        mine = jnp.minimum(step, CHUNKS - 1)
        for k in range(ITERS):
            plus, minus, across = (chunk(link, k, came) for link in (PLUS, MINUS, ACROSS))
            root, first_turn, second_turn, near = (turns[k, n] == 1 for n in range(4))
            staging[slot, PLUS, k] = jnp.where(
                root, chunk(OWN, 0, mine), jnp.where(first_turn, across, plus))
            staging[slot, MINUS, k] = jnp.where(
                root, chunk(OWN, 1, mine), jnp.where(second_turn, across, minus))
            staging[slot, ACROSS, k] = jnp.where(
                root, chunk(OWN, 2, mine), jnp.where(near, plus, minus))
        for link, where in links:
            hop(link, where, step, slot).start()

    for step in range(STEPS - LAG, STEPS):
        for link, _ in links:
            arrival(link, step, step % SLOTS).wait()
    for step in range(STEPS - SLOTS, STEPS):
        for link, where in links:
            hop(link, where, step, step % SLOTS).wait_send()

    dual_step, primal_step, extrapolate = steps[0], steps[1], steps[2]
    rows_local = u.shape[1] // WIDTH
    column = lax.broadcasted_iota(jnp.int32, (WIDTH, 128), 0)
    inner = column < WIDTH - 1
    top = jnp.full((WIDTH, 128), tile) == 0
    bottom = jnp.full((WIDTH, 128), tile) == tiles - 1

    def fluxes(row, under, cut):
        across = jnp.where(inner, pltpu.roll(row, WIDTH - 1, 0) - row, 0.0)
        drop = under - row
        if cut is not None:
            drop = jnp.where(cut, 0.0, drop)
        inverse = 1.0 / jnp.sqrt(across * across + drop * drop + 1.0)
        return across * inverse, drop * inverse

    def smooth(source, m, target):
        for copy in halo_copies(source, m):
            copy.wait()
        flux[...] = jnp.where(top, 0.0, fluxes(above[m], source[pl.ds(0, WIDTH), :], None)[1])

        def one(start, under, cut):
            row = source[pl.ds(start, WIDTH), :]
            right, drop = fluxes(row, under, cut)
            div = right - pltpu.roll(right, 1, 0) + drop - flux[...]
            flux[...] = drop
            target[pl.ds(start, WIDTH), :] = row + primal_step * PENALTY * div

        @pl.loop(0, rows_local - 1)
        def _(r):
            start = pl.multiple_of(r * WIDTH, WIDTH)
            one(start, source[pl.ds(pl.multiple_of(start + WIDTH, WIDTH), WIDTH), :], None)

        one((rows_local - 1) * WIDTH, below[m], bottom)

    smooth(image, 0, u.at[0])

    pairs = blocks // 2
    for k in range(ITERS):
        now = u.at[k]
        for copy in halo_copies(now, k + 1):
            copy.start()
        fwd[k] = jnp.zeros((256, 128), F32)

        @pl.loop(0, pairs)
        def _(q, now=now, k=k):
            def part(b):
                return jnp.concatenate([
                    recv[base[k, tree, 0], base[k, tree, 1], base[k, tree, 2] + (b * COUNTS[tree] + n)]
                    for tree in range(3) for n in range(COUNTS[tree])], axis=0)

            block = jnp.concatenate([part(2 * q), part(2 * q + 1)], axis=1)
            p_high, p_low = halves(block)
            high[q] = p_high
            low[q] = p_low
            x_high, x_low = halves(now[pl.ds(pl.multiple_of(q * 256, 256), 256), :])
            both = matmul(p_high, jnp.concatenate([x_high, x_low], axis=1), ((1,), (0,)))
            rest = matmul(p_low, x_high, ((1,), (0,)))
            fwd[k] += both[:, :128] + (both[:, 128:] + rest)

        def share(d, k=k):
            to = lax.rem(tile + d, tiles)
            return pltpu.make_async_remote_copy(
                fwd.at[k, pl.ds(pl.multiple_of(to * 16, 16), 16)], shares.at[k, d - 1],
                sum_send.at[k, d - 1], sum_recv.at[k, d - 1],
                device_id={"tile": to}, device_id_type=MESH)

        for d in range(1, tiles):
            share(d).start()

        smooth(now, k + 1, w)

        total = fwd[k, pl.ds(pl.multiple_of(tile * 16, 16), 16), :]
        for d in range(1, tiles):
            share(d).wait()
            total = total + shares[k, d - 1]
        current = jnp.zeros((16, 128), F32)
        for j in range(k):
            current = jnp.where(again[k, j] == 1, duals[j], current)
        updated = (current + dual_step * total - dual_step * measured[k]) / (1.0 + dual_step)
        duals[k] = updated
        change_own[k] = updated - current

        def spread(d, k=k):
            return pltpu.make_async_remote_copy(
                change_own.at[k], changes.at[k, d - 1],
                all_send.at[k, d - 1], all_recv.at[k, d - 1],
                device_id={"tile": lax.rem(tile + d, tiles)}, device_id_type=MESH)

        for d in range(1, tiles):
            spread(d).start()
        for d in range(1, tiles):
            spread(d).wait()
        fwd[k, pl.ds(pl.multiple_of(tile * 16, 16), 16), :] = change_own[k]
        for d in range(1, tiles):
            came = lax.rem(tile + tiles - d, tiles)
            fwd[k, pl.ds(pl.multiple_of(came * 16, 16), 16), :] = changes[k, d - 1]
        c_high, c_low = halves(fwd[k])
        c_both = jnp.concatenate([c_high, c_low], axis=1)

        @pl.loop(0, pairs)
        def _(q, k=k, c_high=c_high, c_both=c_both):
            both = matmul(high[q], c_both, ((0,), (0,)))
            rest = matmul(low[q], c_high, ((0,), (0,)))
            adjoint = both[:, :128] + (both[:, 128:] + rest)
            at = pl.ds(pl.multiple_of(q * 256, 256), 256)
            gathered = adjoint if k == 0 else acc[at, :] + adjoint
            if k < ITERS - 1:
                acc[at, :] = gathered
            pushed = gathered + extrapolate * 16.0 * adjoint
            result = w[at, :] - primal_step * pushed
            if k < ITERS - 1:
                u[k + 1, at, :] = result
            else:
                out[at, :] = result


def routes(order):
    col = lax.axis_index("col")
    rail, z = col // RING, col % RING
    i, same = (z - order % RING) % RING, rail == order // RING
    root = same & (i == 0)
    flags = jnp.stack([
        root,
        ~same & ((i == 0) | (i == 4)),
        ~same & ((i == 0) | (i == 5)),
        i <= 4,
    ], axis=1)
    turns = jnp.broadcast_to(
        flags.astype(jnp.int32)[:, :, None, None, None], (ITERS, 4, CHUNK, 8, 128))
    link = jnp.stack([
        jnp.where(same | (i == 0) | (i > 4), PLUS, ACROSS),
        jnp.where(same | (i <= 4), MINUS, ACROSS),
        jnp.where(same | (i == 0), ACROSS, jnp.where(i <= 4, PLUS, MINUS)),
    ], axis=1)
    depth = jnp.stack([
        jnp.where(same, i, jnp.where(i == 0, 9, i + 1)),
        jnp.where(same, 8 - i, 9 - i),
        jnp.where(same, jnp.where(i <= 4, i + 2, 10 - i), jnp.where(i <= 4, i + 1, 9 - i)),
    ], axis=1)
    k, tree = jnp.arange(ITERS)[:, None], jnp.arange(3)[None, :]
    mine = root[:, None]
    base = jnp.stack([
        jnp.where(mine, OWN, link),
        jnp.where(mine, tree, k),
        jnp.where(mine, 0, (depth - 1) * (LAG * CHUNK)),
    ], axis=2)
    again = jnp.broadcast_to(
        (order[:, None] == order[None, :]).astype(jnp.int32)[:, :, None, None],
        (ITERS, ITERS, 16, 128))
    return base.astype(jnp.int32), turns, again


def per_device(initial_image, panels, sinogram, subset_order, step_sizes):
    pixels, channels = initial_image.shape
    rays = sinogram.shape[1]
    tiles = lax.axis_size("tile")
    measured = jnp.stack([
        lax.dynamic_index_in_dim(sinogram, subset_order[k], 0, keepdims=False)
        for k in range(ITERS)])
    base, turns, again = routes(subset_order)
    tiled = panels.reshape(panels.shape[0], panels.shape[1] // 8, 8, panels.shape[2])
    vmem = pl.BlockSpec(memory_space=pltpu.VMEM)
    smem = pl.BlockSpec(memory_space=pltpu.SMEM)
    dma = pltpu.SemaphoreType.DMA
    blocks = panels.shape[2] // 128
    image, updates = pl.pallas_call(
        kernel,
        out_shape=(jax.ShapeDtypeStruct((pixels, channels), F32),
                   jax.ShapeDtypeStruct((ITERS, rays, channels), F32)),
        in_specs=[smem, smem, vmem, pl.BlockSpec(memory_space=pl.ANY), vmem, vmem, vmem],
        out_specs=(vmem, vmem),
        scratch_shapes=[
            pltpu.VMEM((4, ITERS, STEPS * CHUNK, 8, 128), F32),
            pltpu.VMEM((SLOTS, 3, ITERS, CHUNK, 8, 128), F32),
            pltpu.VMEM((ITERS, pixels, channels), F32),
            pltpu.VMEM((pixels, channels), F32),
            pltpu.VMEM((pixels, channels), F32),
            pltpu.VMEM((blocks // 2, 256, 256), BF16),
            pltpu.VMEM((blocks // 2, 256, 256), BF16),
            pltpu.VMEM((ITERS + 1, WIDTH, channels), F32),
            pltpu.VMEM((ITERS + 1, WIDTH, channels), F32),
            pltpu.VMEM((WIDTH, channels), F32),
            pltpu.VMEM((ITERS, rays * tiles, channels), F32),
            pltpu.VMEM((ITERS, tiles - 1, rays, channels), F32),
            pltpu.VMEM((ITERS, rays, channels), F32),
            pltpu.VMEM((ITERS, tiles - 1, rays, channels), F32),
            dma((SLOTS, 3)), dma((SLOTS, 3)), dma((3, blocks)),
            dma((ITERS + 1, 2)), dma((ITERS + 1, 2)),
            dma((ITERS, tiles - 1)), dma((ITERS, tiles - 1)),
            dma((ITERS, tiles - 1)), dma((ITERS, tiles - 1)),
        ],
        compiler_params=pltpu.CompilerParams(
            collective_id=0, has_side_effects=True, vmem_limit_bytes=62 * 1024 * 1024),
    )(base, step_sizes, initial_image, tiled, measured, turns, again)
    duals = jnp.zeros(sinogram.shape, F32)
    for k in range(ITERS):
        duals = lax.dynamic_update_index_in_dim(duals, updates[k], subset_order[k], 0)
    return image, duals


def solution(mesh):
    in_specs = (P("tile", "col"), P("col", None, "tile"), P(None, "tile", "col"), P(), P())
    out_specs = (P("tile", "col"), P(None, "tile", "col"))
    return jax.shard_map(
        per_device, mesh=mesh, in_specs=in_specs, out_specs=out_specs, check_vma=False
    )
```

```python
import jax
import jax.numpy as jnp
from jax import lax
from jax.experimental import pallas as pl
from jax.experimental.pallas import tpu as pltpu
from jax.sharding import PartitionSpec as P

MESH = pl.DeviceIdType.MESH
WIDTH = 512
ITERS = 3
PENALTY = 0.2
RING = 8
LAG = 7
COUNTS = (11, 11, 10)
CHUNK = 2
CHUNKS = 176
STEPS = CHUNKS + 8 * LAG
SLOTS = 2 * LAG
F32 = jnp.float32
BF16 = jnp.bfloat16
DEEP = 1024
PLUS, MINUS, ACROSS, OWN = 0, 1, 2, 3


def halves(x):
    high = x.astype(BF16)
    return high, (x - high.astype(F32)).astype(BF16)


def matmul(a, b, dims):
    return lax.dot_general(a, b, (dims, ((), ())), preferred_element_type=F32)


def kernel(order, steps, image, panel, sinogram, out, duals,
           recv, staging, turns, updates, u, w, acc, high, low, above, below, flux,
           fwd, shares, changes,
           recv_sem, send_sem, own_sem, halo_send, halo_recv, sum_send, sum_recv, all_send, all_recv):
    col, tile = lax.axis_index("col"), lax.axis_index("tile")
    tiles = lax.axis_size("tile")
    rail, z = col // RING, lax.rem(col, RING)
    up = rail * RING + lax.rem(z + 1, RING)
    down = rail * RING + lax.rem(z + RING - 1, RING)
    partner = (1 - rail) * RING + z
    next_tile, prev_tile = lax.rem(tile + 1, tiles), lax.rem(tile + tiles - 1, tiles)
    links = ((PLUS, up), (MINUS, down), (ACROSS, partner))

    blocks = panel.shape[3] // 128
    def own_copy(tree, block):
        count = COUNTS[tree]
        return pltpu.make_async_copy(
            panel.at[0, pl.ds(sum(COUNTS[:tree]), count), :,
                     pl.ds(pl.multiple_of(block * 128, 128), 128)],
            recv.at[OWN, tree, pl.ds(block * count, count)],
            own_sem.at[tree, block],
        )

    for tree in range(3):
        @pl.loop(0, blocks)
        def _(block, tree=tree):
            own_copy(tree, block).start()

    barrier = pltpu.get_barrier_semaphore()
    for _, where in links:
        pl.semaphore_signal(barrier, inc=1, device_id={"col": where}, device_id_type=MESH)
    for d in range(1, tiles):
        pl.semaphore_signal(
            barrier, inc=1, device_id={"tile": lax.rem(tile + d, tiles)}, device_id_type=MESH)
    pl.semaphore_wait(barrier, tiles + 2)

    def halo_copies(source, m):
        last = source.shape[0] - WIDTH
        return (
            pltpu.make_async_remote_copy(
                source.at[pl.ds(0, WIDTH)], below.at[m], halo_send.at[m, 0], halo_recv.at[m, 0],
                device_id={"tile": prev_tile}, device_id_type=MESH),
            pltpu.make_async_remote_copy(
                source.at[pl.ds(last, WIDTH)], above.at[m], halo_send.at[m, 1], halo_recv.at[m, 1],
                device_id={"tile": next_tile}, device_id_type=MESH),
        )

    for copy in halo_copies(image, 0):
        copy.start()

    early = 2
    for tree in range(3):
        for block in range(early):
            own_copy(tree, block).wait()

    plans = []
    for k in range(ITERS):
        i = lax.rem(z - lax.rem(order[k], RING) + RING, RING)
        same = lax.div(order[k], RING) == rail
        root = same & (i == 0)
        flags = (root, ~same & ((i == 0) | (i == 4)), ~same & ((i == 0) | (i == 5)), i <= 4)
        for n, flag in enumerate(flags):
            turns[k, n] = jnp.full((8, 128), flag.astype(jnp.int32))
        link = (
            jnp.where(same | (i == 0) | (i > 4), PLUS, ACROSS),
            jnp.where(same | (i <= 4), MINUS, ACROSS),
            jnp.where(same | (i == 0), ACROSS, jnp.where(i <= 4, PLUS, MINUS)),
        )
        depth = (
            jnp.where(same, i, jnp.where(i == 0, 9, i + 1)),
            jnp.where(same, 8 - i, 9 - i),
            jnp.where(same, jnp.where(i <= 4, i + 2, 10 - i), jnp.where(i <= 4, i + 1, 9 - i)),
        )
        plans.append([
            (jnp.where(root, OWN, link[tree]), jnp.where(root, tree, k),
             jnp.where(root, 0, (depth[tree] - 1) * (LAG * CHUNK)))
            for tree in range(3)])

    def hop(link, where, step, slot):
        return pltpu.make_async_remote_copy(
            staging.at[slot, link],
            recv.at[link, :, pl.ds(step * CHUNK, CHUNK)],
            send_sem.at[slot, link], recv_sem.at[slot, link],
            device_id={"col": where}, device_id_type=MESH)

    def arrival(link, step, slot):
        ref = recv.at[link, :, pl.ds(step * CHUNK, CHUNK)]
        return pltpu.make_async_copy(ref, ref, recv_sem.at[slot, link])

    def chunk(link, k, step):
        return recv[link, k, pl.ds(step * CHUNK, CHUNK)]

    for step in range(LAG):
        for tree, (link, where) in enumerate(links):
            for k in range(ITERS):
                staging[step, link, k] = chunk(OWN, tree, step)
        for link, where in links:
            hop(link, where, step, step).start()

    for tree in range(3):
        @pl.loop(early, blocks)
        def _(block, tree=tree):
            own_copy(tree, block).wait()

    def relay(step):
        slot = lax.rem(step, SLOTS)
        came = step - LAG
        for link, _ in links:
            arrival(link, came, lax.rem(came, SLOTS)).wait()

        @pl.when(step >= SLOTS)
        def _():
            for link, where in links:
                hop(link, where, step - SLOTS, slot).wait_send()

        mine = jnp.minimum(step, CHUNKS - 1)
        for k in range(ITERS):
            plus, minus, across = (chunk(link, k, came) for link in (PLUS, MINUS, ACROSS))
            root, first_turn, second_turn, near = (
                jnp.broadcast_to(turns[k, n] == 1, (CHUNK, 8, 128)) for n in range(4))
            staging[slot, PLUS, k] = jnp.where(
                root, chunk(OWN, 0, mine), jnp.where(first_turn, across, plus))
            staging[slot, MINUS, k] = jnp.where(
                root, chunk(OWN, 1, mine), jnp.where(second_turn, across, minus))
            staging[slot, ACROSS, k] = jnp.where(
                root, chunk(OWN, 2, mine), jnp.where(near, plus, minus))
        for link, where in links:
            hop(link, where, step, slot).start()

    dual_step, primal_step, extrapolate = steps[0], steps[1], steps[2]
    rows_local = u.shape[1] // WIDTH
    column = lax.broadcasted_iota(jnp.int32, (WIDTH, 128), 0)
    inner = column < WIDTH - 1
    top = jnp.full((WIDTH, 128), tile) == 0
    bottom = jnp.full((WIDTH, 128), tile) == tiles - 1

    def fluxes(row, under, cut):
        across = jnp.where(inner, pltpu.roll(row, WIDTH - 1, 0) - row, 0.0)
        drop = under - row
        if cut is not None:
            drop = jnp.where(cut, 0.0, drop)
        inverse = 1.0 / jnp.sqrt(across * across + drop * drop + 1.0)
        return across * inverse, drop * inverse

    def smooth_begin(source, m):
        for copy in halo_copies(source, m):
            copy.wait()
        flux[...] = jnp.where(top, 0.0, fluxes(above[m], source[pl.ds(0, WIDTH), :], None)[1])

    def smooth_row(source, target, start, under, cut):
        row = source[pl.ds(start, WIDTH), :]
        right, drop = fluxes(row, under, cut)
        div = right - pltpu.roll(right, 1, 0) + drop - flux[...]
        flux[...] = drop
        target[pl.ds(start, WIDTH), :] = row + primal_step * PENALTY * div

    def smooth(source, m, target, beside=lambda r: None):
        smooth_begin(source, m)

        @pl.loop(0, rows_local - 1)
        def _(r):
            start = pl.multiple_of(r * WIDTH, WIDTH)
            under = source[pl.ds(pl.multiple_of(start + WIDTH, WIDTH), WIDTH), :]
            smooth_row(source, target, start, under, None)
            beside(r)

        smooth_row(source, target, (rows_local - 1) * WIDTH, below[m], bottom)

    def row_at(source, r):
        return source[pl.ds(pl.multiple_of(r * WIDTH, WIDTH), WIDTH), :]

    def smooth_inner(source, target):
        flux[...] = fluxes(row_at(source, 0), row_at(source, 1), None)[1]

        @pl.loop(1, rows_local - 1)
        def _(r):
            smooth_row(source, target, pl.multiple_of(r * WIDTH, WIDTH), row_at(source, r + 1), None)

    def smooth_edges(source, m, target):
        for copy in halo_copies(source, m):
            copy.wait()
        smooth_row(source, target, (rows_local - 1) * WIDTH, below[m], bottom)
        flux[...] = jnp.where(top, 0.0, fluxes(above[m], row_at(source, 0), None)[1])
        smooth_row(source, target, 0, row_at(source, 1), None)

    settled = LAG + 24
    pl.loop(LAG, settled)(relay)
    smooth(image, 0, u.at[0], lambda r: relay(settled + r))
    pl.loop(settled + rows_local - 1, STEPS)(relay)
    for step in range(STEPS - LAG, STEPS):
        for link, _ in links:
            arrival(link, step, step % SLOTS).wait()
    for step in range(STEPS - SLOTS, STEPS):
        for link, where in links:
            hop(link, where, step, step % SLOTS).wait_send()

    pairs = blocks // 2

    def gather(k, begin, end):
        plan = plans[k]

        @pl.loop(begin, end)
        def _(q):
            def part(b):
                return jnp.concatenate([
                    recv[plan[tree][0], plan[tree][1], plan[tree][2] + (b * COUNTS[tree] + n)]
                    for tree in range(3) for n in range(COUNTS[tree])], axis=0)

            at = pl.ds(pl.multiple_of(q * 256, 256), 256)
            p_high, p_low = halves(jnp.concatenate([part(2 * q), part(2 * q + 1)], axis=1))
            high[k % 2, :, at] = p_high
            low[k % 2, :, at] = p_low

    gather(0, 0, pairs)
    for k in range(ITERS):
        now = u.at[k]
        fwd[k] = jnp.zeros((256, 128), F32)

        @pl.loop(0, blocks * 128 // DEEP)
        def _(q, now=now, k=k):
            at = pl.ds(pl.multiple_of(q * DEEP, DEEP), DEEP)
            x_high, x_low = halves(now[at, :])
            p_high = high[k % 2, :, at]
            both = matmul(p_high, jnp.concatenate([x_high, x_low], axis=1), ((1,), (0,)))
            rest = matmul(low[k % 2, :, at], x_high, ((1,), (0,)))
            fwd[k] += both[:, :128] + (both[:, 128:] + rest)

        def share(d, k=k):
            to = lax.rem(tile + d, tiles)
            return pltpu.make_async_remote_copy(
                fwd.at[k, pl.ds(pl.multiple_of(to * 16, 16), 16)], shares.at[k, d - 1],
                sum_send.at[k, d - 1], sum_recv.at[k, d - 1],
                device_id={"tile": to}, device_id_type=MESH)

        for d in range(1, tiles):
            share(d).start()
        for copy in halo_copies(now, k + 1):
            copy.start()

        if k < ITERS - 1:
            gather(k + 1, 0, pairs)

        mine = pl.ds(pl.multiple_of(tile * 16, 16), 16)
        total = fwd[k, mine, :]
        for d in range(1, tiles):
            share(d).wait()
            total = total + shares[k, d - 1]
        current = jnp.zeros((16, 128), F32)
        for j in range(k):
            again = jnp.full((16, 128), (order[j] == order[k]).astype(jnp.int32)) == 1
            current = jnp.where(again, updates[j], current)
        measured = sinogram[order[k]]
        updated = (current + dual_step * total - dual_step * measured) / (1.0 + dual_step)
        updates[k] = updated
        changes[k, mine, :] = updated - current

        def spread(d, k=k, mine=mine):
            return pltpu.make_async_remote_copy(
                changes.at[k, mine], changes.at[k, mine],
                all_send.at[k, d - 1], all_recv.at[k, d - 1],
                device_id={"tile": lax.rem(tile + d, tiles)}, device_id_type=MESH)

        def spread_to_me(d, k=k):
            rows = changes.at[k, pl.ds(
                pl.multiple_of(lax.rem(tile + tiles - d, tiles) * 16, 16), 16)]
            return pltpu.make_async_copy(rows, rows, all_recv.at[k, d - 1])

        for d in range(1, tiles):
            spread(d).start()
        smooth_inner(now, w)
        for d in range(1, tiles):
            spread(d).wait_send()
            spread_to_me(d).wait()
        c_high, c_low = halves(changes[k])
        c_both = jnp.concatenate([c_high, c_low], axis=1)

        def push(q, k=k, c_high=c_high, c_both=c_both):
            at = pl.ds(pl.multiple_of(q * WIDTH, WIDTH), WIDTH)
            both = matmul(high[k % 2, :, at], c_both, ((0,), (0,)))
            rest = matmul(low[k % 2, :, at], c_high, ((0,), (0,)))
            adjoint = both[:, :128] + (both[:, 128:] + rest)
            gathered = adjoint if k == 0 else acc[at, :] + adjoint
            if k < ITERS - 1:
                acc[at, :] = gathered
            pushed = gathered + extrapolate * 16.0 * adjoint
            result = w[at, :] - primal_step * pushed
            if k < ITERS - 1:
                u[k + 1, at, :] = result
            else:
                out[at, :] = result

        pl.loop(1, rows_local - 1)(push)
        smooth_edges(now, k + 1, w)
        pl.loop(0, rows_local, step=rows_local - 1)(push)

    for subset in range(duals.shape[0]):
        final = jnp.zeros((16, 128), F32)
        for k in range(ITERS):
            here = jnp.full((16, 128), (order[k] == subset).astype(jnp.int32)) == 1
            final = jnp.where(here, updates[k], final)
        duals[subset] = final


def per_device(initial_image, panels, sinogram, subset_order, step_sizes):
    pixels, channels = initial_image.shape
    rays = sinogram.shape[1]
    tiles = lax.axis_size("tile")
    tiled = panels.reshape(panels.shape[0], panels.shape[1] // 8, 8, panels.shape[2])
    vmem = pl.BlockSpec(memory_space=pltpu.VMEM)
    smem = pl.BlockSpec(memory_space=pltpu.SMEM)
    dma = pltpu.SemaphoreType.DMA
    blocks = panels.shape[2] // 128
    return pl.pallas_call(
        kernel,
        out_shape=(jax.ShapeDtypeStruct((pixels, channels), F32),
                   jax.ShapeDtypeStruct(sinogram.shape, F32)),
        in_specs=[smem, smem, vmem, pl.BlockSpec(memory_space=pl.ANY), vmem],
        out_specs=(vmem, vmem),
        scratch_shapes=[
            pltpu.VMEM((4, ITERS, STEPS * CHUNK, 8, 128), F32),
            pltpu.VMEM((SLOTS, 3, ITERS, CHUNK, 8, 128), F32),
            pltpu.VMEM((ITERS, 4, 8, 128), jnp.int32),
            pltpu.VMEM((ITERS, rays, channels), F32),
            pltpu.VMEM((ITERS, pixels, channels), F32),
            pltpu.VMEM((pixels, channels), F32),
            pltpu.VMEM((pixels, channels), F32),
            pltpu.VMEM((2, rays * tiles, blocks * 128), BF16),
            pltpu.VMEM((2, rays * tiles, blocks * 128), BF16),
            pltpu.VMEM((ITERS + 1, WIDTH, channels), F32),
            pltpu.VMEM((ITERS + 1, WIDTH, channels), F32),
            pltpu.VMEM((WIDTH, channels), F32),
            pltpu.VMEM((ITERS, rays * tiles, channels), F32),
            pltpu.VMEM((ITERS, tiles - 1, rays, channels), F32),
            pltpu.VMEM((ITERS, rays * tiles, channels), F32),
            dma((SLOTS, 3)), dma((SLOTS, 3)), dma((3, blocks)),
            dma((ITERS + 1, 2)), dma((ITERS + 1, 2)),
            dma((ITERS, tiles - 1)), dma((ITERS, tiles - 1)),
            dma((ITERS, tiles - 1)), dma((ITERS, tiles - 1)),
        ],
        compiler_params=pltpu.CompilerParams(
            collective_id=0, has_side_effects=True, vmem_limit_bytes=62 * 1024 * 1024),
    )(subset_order, step_sizes, initial_image, tiled, sinogram)


def solution(mesh):
    in_specs = (P("tile", "col"), P("col", None, "tile"), P(None, "tile", "col"), P(), P())
    out_specs = (P("tile", "col"), P(None, "tile", "col"))
    return jax.shard_map(
        per_device, mesh=mesh, in_specs=in_specs, out_specs=out_specs, check_vma=False
    )
```

```python
import jax
import jax.numpy as jnp
from jax import lax
from jax.experimental import pallas as pl
from jax.experimental.pallas import tpu as pltpu
from jax.sharding import PartitionSpec as P

MESH = pl.DeviceIdType.MESH
WIDTH = 512
ITERS = 3
PENALTY = 0.2
RING = 8
LAG = 7
COUNTS = (11, 11, 10)
CHUNK = 2
CHUNKS = 176
STEPS = CHUNKS + 8 * LAG
SLOTS = 2 * LAG
F32 = jnp.float32
BF16 = jnp.bfloat16
DEEP = 1024
PLUS, MINUS, ACROSS, OWN = 0, 1, 2, 3


def halves(x):
    high = x.astype(BF16)
    return high, (x - high.astype(F32)).astype(BF16)


def matmul(a, b, dims):
    return lax.dot_general(a, b, (dims, ((), ())), preferred_element_type=F32)


def kernel(order, steps, image, panel, sinogram, out, duals,
           recv, staging, turns, updates, u, w, acc, high, low, above, below, flux,
           fwd, shares, changes,
           recv_sem, send_sem, own_sem, halo_send, halo_recv, sum_send, sum_recv, all_send, all_recv):
    col, tile = lax.axis_index("col"), lax.axis_index("tile")
    tiles = lax.axis_size("tile")
    rail, z = col // RING, lax.rem(col, RING)
    up = rail * RING + lax.rem(z + 1, RING)
    down = rail * RING + lax.rem(z + RING - 1, RING)
    partner = (1 - rail) * RING + z
    next_tile, prev_tile = lax.rem(tile + 1, tiles), lax.rem(tile + tiles - 1, tiles)
    links = ((PLUS, up), (MINUS, down), (ACROSS, partner))

    blocks = panel.shape[3] // 128
    def own_copy(tree, block):
        count = COUNTS[tree]
        return pltpu.make_async_copy(
            panel.at[0, pl.ds(sum(COUNTS[:tree]), count), :,
                     pl.ds(pl.multiple_of(block * 128, 128), 128)],
            recv.at[OWN, tree, pl.ds(block * count, count)],
            own_sem.at[tree, block],
        )

    for tree in range(3):
        @pl.loop(0, blocks)
        def _(block, tree=tree):
            own_copy(tree, block).start()

    barrier = pltpu.get_barrier_semaphore()
    for _, where in links:
        pl.semaphore_signal(barrier, inc=1, device_id={"col": where}, device_id_type=MESH)
    for d in range(1, tiles):
        pl.semaphore_signal(
            barrier, inc=1, device_id={"tile": lax.rem(tile + d, tiles)}, device_id_type=MESH)
    pl.semaphore_wait(barrier, tiles + 2)

    def halo_copy(source, m, side):
        where, row, to = (
            (prev_tile, 0, below), (next_tile, source.shape[0] - WIDTH, above))[side]
        return pltpu.make_async_remote_copy(
            source.at[pl.ds(row, WIDTH)], to.at[m], halo_send.at[m, side], halo_recv.at[m, side],
            device_id={"tile": where}, device_id_type=MESH)

    def halo_copies(source, m):
        return halo_copy(source, m, 0), halo_copy(source, m, 1)

    for copy in halo_copies(image, 0):
        copy.start()

    early = 2
    for tree in range(3):
        for block in range(early):
            own_copy(tree, block).wait()

    plans = []
    for k in range(ITERS):
        i = lax.rem(z - lax.rem(order[k], RING) + RING, RING)
        same = lax.div(order[k], RING) == rail
        root = same & (i == 0)
        flags = (root, ~same & ((i == 0) | (i == 4)), ~same & ((i == 0) | (i == 5)), i <= 4)
        for n, flag in enumerate(flags):
            turns[k, n] = jnp.full((8, 128), flag.astype(jnp.int32))
        link = (
            jnp.where(same | (i == 0) | (i > 4), PLUS, ACROSS),
            jnp.where(same | (i <= 4), MINUS, ACROSS),
            jnp.where(same | (i == 0), ACROSS, jnp.where(i <= 4, PLUS, MINUS)),
        )
        depth = (
            jnp.where(same, i, jnp.where(i == 0, 9, i + 1)),
            jnp.where(same, 8 - i, 9 - i),
            jnp.where(same, jnp.where(i <= 4, i + 2, 10 - i), jnp.where(i <= 4, i + 1, 9 - i)),
        )
        plans.append([
            (jnp.where(root, OWN, link[tree]), jnp.where(root, tree, k),
             jnp.where(root, 0, (depth[tree] - 1) * (LAG * CHUNK)))
            for tree in range(3)])

    def hop(link, where, step, slot):
        return pltpu.make_async_remote_copy(
            staging.at[slot, link],
            recv.at[link, :, pl.ds(step * CHUNK, CHUNK)],
            send_sem.at[slot, link], recv_sem.at[slot, link],
            device_id={"col": where}, device_id_type=MESH)

    def arrival(link, step, slot):
        ref = recv.at[link, :, pl.ds(step * CHUNK, CHUNK)]
        return pltpu.make_async_copy(ref, ref, recv_sem.at[slot, link])

    def chunk(link, k, step):
        return recv[link, k, pl.ds(step * CHUNK, CHUNK)]

    for step in range(LAG):
        for tree, (link, where) in enumerate(links):
            for k in range(ITERS):
                staging[step, link, k] = chunk(OWN, tree, step)
        for link, where in links:
            hop(link, where, step, step).start()

    for tree in range(3):
        @pl.loop(early, blocks)
        def _(block, tree=tree):
            own_copy(tree, block).wait()

    def relay(step):
        slot = lax.rem(step, SLOTS)
        came = step - LAG
        for link, _ in links:
            arrival(link, came, lax.rem(came, SLOTS)).wait()

        @pl.when(step >= SLOTS)
        def _():
            for link, where in links:
                hop(link, where, step - SLOTS, slot).wait_send()

        mine = jnp.minimum(step, CHUNKS - 1)
        for k in range(ITERS):
            plus, minus, across = (chunk(link, k, came) for link in (PLUS, MINUS, ACROSS))
            root, first_turn, second_turn, near = (
                jnp.broadcast_to(turns[k, n] == 1, (CHUNK, 8, 128)) for n in range(4))
            staging[slot, PLUS, k] = jnp.where(
                root, chunk(OWN, 0, mine), jnp.where(first_turn, across, plus))
            staging[slot, MINUS, k] = jnp.where(
                root, chunk(OWN, 1, mine), jnp.where(second_turn, across, minus))
            staging[slot, ACROSS, k] = jnp.where(
                root, chunk(OWN, 2, mine), jnp.where(near, plus, minus))
        for link, where in links:
            hop(link, where, step, slot).start()

    dual_step, primal_step, extrapolate = steps[0], steps[1], steps[2]
    rows_local = u.shape[1] // WIDTH
    column = lax.broadcasted_iota(jnp.int32, (WIDTH, 128), 0)
    inner = column < WIDTH - 1
    top = jnp.full((WIDTH, 128), tile) == 0
    bottom = jnp.full((WIDTH, 128), tile) == tiles - 1

    def fluxes(row, under, cut):
        across = jnp.where(inner, pltpu.roll(row, WIDTH - 1, 0) - row, 0.0)
        drop = under - row
        if cut is not None:
            drop = jnp.where(cut, 0.0, drop)
        inverse = lax.rsqrt(across * across + drop * drop + 1.0)
        return across * inverse, drop * inverse

    def smooth_begin(source, m):
        for copy in halo_copies(source, m):
            copy.wait()
        flux[...] = jnp.where(top, 0.0, fluxes(above[m], source[pl.ds(0, WIDTH), :], None)[1])

    def smooth_row(source, target, start, under, cut):
        row = source[pl.ds(start, WIDTH), :]
        right, drop = fluxes(row, under, cut)
        div = right - pltpu.roll(right, 1, 0) + drop - flux[...]
        flux[...] = drop
        target[pl.ds(start, WIDTH), :] = row + primal_step * PENALTY * div

    def smooth(source, m, target, beside=lambda r: None):
        smooth_begin(source, m)

        @pl.loop(0, rows_local - 1)
        def _(r):
            start = pl.multiple_of(r * WIDTH, WIDTH)
            under = source[pl.ds(pl.multiple_of(start + WIDTH, WIDTH), WIDTH), :]
            smooth_row(source, target, start, under, None)
            beside(r)

        smooth_row(source, target, (rows_local - 1) * WIDTH, below[m], bottom)

    def row_at(source, r):
        return source[pl.ds(pl.multiple_of(r * WIDTH, WIDTH), WIDTH), :]

    def smooth_inner(source, target):
        flux[...] = fluxes(row_at(source, 0), row_at(source, 1), None)[1]

        @pl.loop(1, rows_local - 1)
        def _(r):
            smooth_row(source, target, pl.multiple_of(r * WIDTH, WIDTH), row_at(source, r + 1), None)

    def smooth_edges(source, m, target):
        for copy in halo_copies(source, m):
            copy.wait()
        smooth_row(source, target, (rows_local - 1) * WIDTH, below[m], bottom)
        flux[...] = jnp.where(top, 0.0, fluxes(above[m], row_at(source, 0), None)[1])
        smooth_row(source, target, 0, row_at(source, 1), None)

    settled = LAG + 96
    pl.loop(LAG, settled)(relay)
    smooth(image, 0, u.at[0], lambda r: relay(settled + r))
    pl.loop(settled + rows_local - 1, STEPS)(relay)
    for step in range(STEPS - LAG, STEPS):
        for link, _ in links:
            arrival(link, step, step % SLOTS).wait()
    for step in range(STEPS - SLOTS, STEPS):
        for link, where in links:
            hop(link, where, step, step % SLOTS).wait_send()

    pairs = blocks // 2

    def gather(k, begin, end):
        plan = plans[k]

        @pl.loop(begin, end)
        def _(q):
            def part(b):
                return jnp.concatenate([
                    recv[plan[tree][0], plan[tree][1], plan[tree][2] + (b * COUNTS[tree] + n)]
                    for tree in range(3) for n in range(COUNTS[tree])], axis=0)

            at = pl.ds(pl.multiple_of(q * 256, 256), 256)
            p_high, p_low = halves(jnp.concatenate([part(2 * q), part(2 * q + 1)], axis=1))
            high[k % 2, :, at] = p_high
            low[k % 2, :, at] = p_low

    gather(0, 0, pairs)
    for k in range(ITERS):
        now = u.at[k]
        fwd[k] = jnp.zeros((256, 128), F32)

        @pl.loop(0, blocks * 128 // DEEP)
        def _(q, now=now, k=k):
            at = pl.ds(pl.multiple_of(q * DEEP, DEEP), DEEP)
            x_high, x_low = halves(now[at, :])
            p_high = high[k % 2, :, at]
            both = matmul(p_high, jnp.concatenate([x_high, x_low], axis=1), ((1,), (0,)))
            rest = matmul(low[k % 2, :, at], x_high, ((1,), (0,)))
            fwd[k] += both[:, :128] + (both[:, 128:] + rest)

        def share(d, k=k):
            to = lax.rem(tile + d, tiles)
            return pltpu.make_async_remote_copy(
                fwd.at[k, pl.ds(pl.multiple_of(to * 16, 16), 16)], shares.at[k, d - 1],
                sum_send.at[k, d - 1], sum_recv.at[k, d - 1],
                device_id={"tile": to}, device_id_type=MESH)

        for d in range(1, tiles):
            share(d).start()
        halo_copy(now, k + 1, 1).start()

        if k < ITERS - 1:
            gather(k + 1, 0, pairs)

        mine = pl.ds(pl.multiple_of(tile * 16, 16), 16)
        total = fwd[k, mine, :]
        for d in range(1, tiles):
            share(d).wait()
            total = total + shares[k, d - 1]
        current = jnp.zeros((16, 128), F32)
        for j in range(k):
            again = jnp.full((16, 128), (order[j] == order[k]).astype(jnp.int32)) == 1
            current = jnp.where(again, updates[j], current)
        measured = sinogram[order[k]]
        updated = (current + dual_step * total - dual_step * measured) / (1.0 + dual_step)
        updates[k] = updated
        changes[k, mine, :] = updated - current

        def spread(d, k=k, mine=mine):
            return pltpu.make_async_remote_copy(
                changes.at[k, mine], changes.at[k, mine],
                all_send.at[k, d - 1], all_recv.at[k, d - 1],
                device_id={"tile": lax.rem(tile + d, tiles)}, device_id_type=MESH)

        def spread_to_me(d, k=k):
            rows = changes.at[k, pl.ds(
                pl.multiple_of(lax.rem(tile + tiles - d, tiles) * 16, 16), 16)]
            return pltpu.make_async_copy(rows, rows, all_recv.at[k, d - 1])

        for d in range(1, tiles):
            spread(d).start()
        halo_copy(now, k + 1, 0).start()
        smooth_inner(now, w)
        for d in range(1, tiles):
            spread(d).wait_send()
            spread_to_me(d).wait()
        c_high, c_low = halves(changes[k])
        c_both = jnp.concatenate([c_high, c_low], axis=1)

        def push(q, k=k, c_high=c_high, c_both=c_both):
            at = pl.ds(pl.multiple_of(q * WIDTH, WIDTH), WIDTH)
            both = matmul(high[k % 2, :, at], c_both, ((0,), (0,)))
            rest = matmul(low[k % 2, :, at], c_high, ((0,), (0,)))
            adjoint = both[:, :128] + (both[:, 128:] + rest)
            gathered = adjoint if k == 0 else acc[at, :] + adjoint
            if k < ITERS - 1:
                acc[at, :] = gathered
            pushed = gathered + extrapolate * 16.0 * adjoint
            result = w[at, :] - primal_step * pushed
            if k < ITERS - 1:
                u[k + 1, at, :] = result
            else:
                out[at, :] = result

        pl.loop(1, rows_local - 1)(push)
        smooth_edges(now, k + 1, w)
        pl.loop(0, rows_local, step=rows_local - 1)(push)

    for subset in range(duals.shape[0]):
        final = jnp.zeros((16, 128), F32)
        for k in range(ITERS):
            here = jnp.full((16, 128), (order[k] == subset).astype(jnp.int32)) == 1
            final = jnp.where(here, updates[k], final)
        duals[subset] = final


def per_device(initial_image, panels, sinogram, subset_order, step_sizes):
    pixels, channels = initial_image.shape
    rays = sinogram.shape[1]
    tiles = lax.axis_size("tile")
    tiled = panels.reshape(panels.shape[0], panels.shape[1] // 8, 8, panels.shape[2])
    vmem = pl.BlockSpec(memory_space=pltpu.VMEM)
    smem = pl.BlockSpec(memory_space=pltpu.SMEM)
    dma = pltpu.SemaphoreType.DMA
    blocks = panels.shape[2] // 128
    return pl.pallas_call(
        kernel,
        out_shape=(jax.ShapeDtypeStruct((pixels, channels), F32),
                   jax.ShapeDtypeStruct(sinogram.shape, F32)),
        in_specs=[smem, smem, vmem, pl.BlockSpec(memory_space=pl.ANY), vmem],
        out_specs=(vmem, vmem),
        scratch_shapes=[
            pltpu.VMEM((4, ITERS, STEPS * CHUNK, 8, 128), F32),
            pltpu.VMEM((SLOTS, 3, ITERS, CHUNK, 8, 128), F32),
            pltpu.VMEM((ITERS, 4, 8, 128), jnp.int32),
            pltpu.VMEM((ITERS, rays, channels), F32),
            pltpu.VMEM((ITERS, pixels, channels), F32),
            pltpu.VMEM((pixels, channels), F32),
            pltpu.VMEM((pixels, channels), F32),
            pltpu.VMEM((2, rays * tiles, blocks * 128), BF16),
            pltpu.VMEM((2, rays * tiles, blocks * 128), BF16),
            pltpu.VMEM((ITERS + 1, WIDTH, channels), F32),
            pltpu.VMEM((ITERS + 1, WIDTH, channels), F32),
            pltpu.VMEM((WIDTH, channels), F32),
            pltpu.VMEM((ITERS, rays * tiles, channels), F32),
            pltpu.VMEM((ITERS, tiles - 1, rays, channels), F32),
            pltpu.VMEM((ITERS, rays * tiles, channels), F32),
            dma((SLOTS, 3)), dma((SLOTS, 3)), dma((3, blocks)),
            dma((ITERS + 1, 2)), dma((ITERS + 1, 2)),
            dma((ITERS, tiles - 1)), dma((ITERS, tiles - 1)),
            dma((ITERS, tiles - 1)), dma((ITERS, tiles - 1)),
        ],
        compiler_params=pltpu.CompilerParams(
            collective_id=0, has_side_effects=True, vmem_limit_bytes=51 * 1024 * 1024),
    )(subset_order, step_sizes, initial_image, tiled, sinogram)


def solution(mesh):
    in_specs = (P("tile", "col"), P("col", None, "tile"), P(None, "tile", "col"), P(), P())
    out_specs = (P("tile", "col"), P(None, "tile", "col"))
    return jax.shard_map(
        per_device, mesh=mesh, in_specs=in_specs, out_specs=out_specs, check_vma=False
    )
```
